32 devices in a mesh: row: 4 (over y, x), col: 8 (over z, core).
Axes of the slice: x: 2, y: 2, z: 4, core: 2. Of those that a mesh axis runs over, the one named last changes fastest.
Arguments:
- docs: bfloat16 [4096, 4, 896], P(('row', 'col')), may hold values from -6 to 6
- routes: int32 [4096, 1], P(('row', 'col')), may hold values from 0 to 31; in each aligned block of 128 rows (0 to 127, 128 to 255, ...) at most 8 rows name the same one
- level_one: float32 [4, 896, 896], P('row', 'col'), may hold values from -6 to 6
- level_two: float32 [8, 896, 896], P('col', 'row'), may hold values from -6 to 6
- moment_one: float32 [4, 896, 896], P('row', 'col'), may hold values from -18 to 18
- moment_two: float32 [8, 896, 896], P('col', 'row'), may hold values from -18 to 18
Outputs:
- new_one: float32 [4, 896, 896], P('row', 'col')
- new_two: float32 [8, 896, 896], P('col', 'row')
- next_moment_one: float32 [4, 896, 896], P('row', 'col')
- next_moment_two: float32 [8, 896, 896], P('col', 'row')
The draws below stay inside these ranges and needn't reach their ends.
Inputs may be any that keep to these rules, and one draw needn't show every extreme that they name: `routes`: each block names one path; among the 128 blocks of one device no path is named more than 8 times, and every path is named by some block.
All inputs are finite; a program needn't handle non-finite values.
Results may differ from the reference program's by a relative error of at most 0.017.
Values may be sent and summed in bfloat16 or wider, within the bound.
A program may use at most 128 MiB of HBM per device.

```python
import math
import jax
import jax.numpy as jnp
import numpy as np
from jax import lax

D = 896
BLOCK = 4
STEPS = 3
DOCS = 128
PATHS = 32
CAP = 8
TOTAL_DOCS = 4096
N_ROW = 4
N_COL = 8


def block_scale(stream_key, dims, shards, smallest, high):
    level, own = 1.0, jax.random.fold_in(stream_key, 6)
    for axis_at, parts in shards:
        heights = jnp.exp(jax.random.uniform(jax.random.fold_in(own, axis_at), (parts,), jnp.float32, smallest / len(shards), high / len(shards)))
        level = level * jnp.repeat(heights, dims[axis_at] // parts).reshape([-1 if axis == axis_at else 1 for axis in range(len(dims))])
    return level


def assign_block(rng, own, number, rows, number_of, top, limit, slope):
    ranking = jax.random.permutation(rng, number_of)
    heavy_load, common = portions_of(number_of, rows * top, limit, slope, True), portions_of(number_of, rows * top, limit, slope, False)
    places = jnp.arange(number_of)

    def named(tallies, rotation):
        used = int((tallies > 0).sum())
        fixed = max(1, used // 4)
        shifted = fixed + (places - fixed + rotation * (used - fixed)) % max(1, number_of - fixed)
        return jnp.zeros((number_of,), jnp.int32).at[ranking[jnp.where(places < fixed, places, shifted)]].set(jnp.asarray(tallies, jnp.int32))

    tallies = jnp.where(number % 4 == 0, named(heavy_load, number // 4), named(common, number - number // 4 - 1))
    mixed = jax.random.permutation(jax.random.fold_in(own, 3), number_of)
    donor, taker = mixed[0:number_of // 2 * 2:2], mixed[1:number_of // 2 * 2:2]
    margin = jnp.minimum(tallies[donor] - 1, limit - tallies[taker]) // 2
    margin = jnp.where((donor == ranking[0]) | (taker == ranking[0]) | (tallies[taker] == 0), 0, jnp.maximum(margin, 0))
    shifted = jax.random.randint(jax.random.fold_in(own, 4), (number_of // 2,), 0, 1 << 20) % (margin + 1)
    tallies = tallies.at[donor].add(-shifted).at[taker].add(shifted)
    items = jnp.searchsorted(jnp.cumsum(tallies), jnp.arange(rows * top), side="right").astype(jnp.int32)
    table = items.reshape(top, rows).T
    table = table[jax.random.permutation(jax.random.fold_in(own, 1), rows)]
    rotation = jax.random.randint(jax.random.fold_in(own, 2), (rows, 1), 0, top)
    return jnp.take_along_axis(table, (jnp.arange(top)[None, :] + rotation) % top, axis=1)


def portions_of(count, total, limit, lean, full):
    portions = [(1 << 20) // math.isqrt(grade ** lean) + 1 for grade in range(1, count + 1)]
    largest = limit if full else min(limit, max(-(-total // count), total * portions[0] // sum(portions)))
    least = 1 if total - largest >= count - 1 else 0
    counts, spare = [largest] + [least] * (count - 1), total - largest - least * (count - 1)
    while spare > 0:
        candidates = [i for i in range(1, count) if counts[i] < largest] or [i for i in range(1, count) if counts[i] < limit]
        whole, remaining = sum([portions[i] for i in candidates]), spare
        for i in candidates:
            more = min(limit - counts[i], max(1, remaining * portions[i] // whole), spare)
            counts[i] = counts[i] + more
            spare = spare - more
    return np.array(counts)


def scatter_about(own_key, extent, scale, bound, shards=(), kind=jnp.bfloat16):
    level = block_scale(own_key, extent, shards, -0.22, 0.18) if shards else 1.0
    entries = jax.random.normal(own_key, extent, jnp.float32) * scale * level
    return jnp.minimum(jnp.maximum(entries, -bound), bound).astype(kind)


def setup_inputs(seed: int = 0) -> dict:
    key_list = jax.random.split(jax.random.key(seed), 7)
    docs = scatter_about(key_list[0], (TOTAL_DOCS, BLOCK, D), 1.0, 6.0, ((0, 32),))
    routes_keys = jax.random.split(jax.random.fold_in(key_list[1], 1), TOTAL_DOCS // DOCS)
    routes_turns = jax.random.permutation(jax.random.fold_in(key_list[1], 3), TOTAL_DOCS // DOCS)
    routes = jax.vmap(lambda own, number: assign_block(jax.random.fold_in(key_list[1], 2), own, number, DOCS, PATHS, 1, CAP, 2))(routes_keys, routes_turns).reshape((TOTAL_DOCS, 1))
    level_one = scatter_about(key_list[2], (N_ROW, D, D), 1.0, 6.0, ((0, 4), (1, 8)), jnp.float32)
    level_two = scatter_about(key_list[3], (N_COL, D, D), 1.0, 6.0, ((0, 8), (1, 4)), jnp.float32)
    moment_one = scatter_about(key_list[4], (N_ROW, D, D), 3.0, 18.0, ((0, 4), (1, 8)), jnp.float32)
    moment_two = scatter_about(key_list[5], (N_COL, D, D), 3.0, 18.0, ((0, 8), (1, 4)), jnp.float32)
    return {"docs": docs, "routes": routes, "level_one": level_one, "level_two": level_two, "moment_one": moment_one, "moment_two": moment_two}


inner_rate = 64.0
outer_rate = 0.7
momentum_decay = 0.9

def normalize(values):
    return values * lax.rsqrt(lax.optimization_barrier(jnp.mean(values * values, axis=-1, keepdims=True)) + 1e-06)

def path_loss(weights, inputs, targets, row_weights):
    first, second = weights
    factor = inputs.shape[-1] ** (-0.5)
    hidden_in = jnp.dot(normalize(inputs).astype(jnp.bfloat16), first.astype(jnp.bfloat16), preferred_element_type=jnp.float32) * factor
    hidden = inputs + jax.nn.silu(hidden_in)
    output = hidden + jnp.dot(normalize(hidden).astype(jnp.bfloat16), second.astype(jnp.bfloat16), preferred_element_type=jnp.float32) * factor
    error = output - targets
    return 0.5 * jnp.sum(row_weights[:, None] * error * error) / jnp.sum(row_weights)

def train_path(first, second, rows, valid):
    width = rows.shape[-1]
    length = rows.shape[-2]
    blocks = rows.reshape(-1, length, width).astype(jnp.float32)
    inputs = blocks[:, :-1].reshape(-1, width)
    targets = blocks[:, 1:].reshape(-1, width)
    row_weights = jnp.repeat(valid.reshape(-1).astype(jnp.float32), length - 1)
    for turn in range(STEPS):
        grads = jax.grad(path_loss)((first, second), inputs, targets, row_weights)
        first = first - inner_rate * grads[0]
        second = second - inner_rate * grads[1]
    return (first, second)

def reference(docs, routes, level_one, level_two, moment_one, moment_two):
    paths = N_ROW * N_COL
    dest = routes[:, 0]
    source_routes = dest.reshape(paths, DOCS)
    onehot = (source_routes[:, :, None] == jnp.arange(paths, dtype=jnp.int32)[None, None, :]).astype(jnp.int32)
    rank = lax.optimization_barrier(jnp.sum(jnp.cumsum(onehot, axis=1) * onehot, axis=2)) - 1
    slot_all = (jnp.arange(paths, dtype=jnp.int32)[:, None] * CAP + rank).reshape(-1).astype(jnp.int32)

    def one_path(carry, path):
        sum_one, sum_two = carry
        place = jnp.where(dest == path, slot_all, paths * CAP).astype(jnp.int32)
        buffer = jnp.zeros((paths * CAP + 1, BLOCK, D), jnp.bfloat16).at[place].add(docs)[:-1]
        valid = jnp.zeros((paths * CAP + 1,), jnp.float32).at[place].add(1.0)[:-1]
        index_one = path // N_COL
        index_two = path % N_COL
        start_one = level_one[index_one]
        start_two = level_two[index_two]
        end_one, end_two = train_path(start_one, start_two, buffer, valid)
        sum_one = sum_one.at[index_one].add(start_one - end_one)
        sum_two = sum_two.at[index_two].add(start_two - end_two)
        return ((sum_one, sum_two), None)
    init = (jnp.zeros((N_ROW, D, D), jnp.float32), jnp.zeros((N_COL, D, D), jnp.float32))
    (sum_one, sum_two), unused = lax.scan(one_path, init, jnp.arange(paths, dtype=jnp.int32))
    delta_one = sum_one / N_COL
    delta_two = sum_two / N_ROW
    next_moment_one = momentum_decay * moment_one + delta_one
    next_moment_two = momentum_decay * moment_two + delta_two
    new_one = level_one - outer_rate * (delta_one + momentum_decay * next_moment_one)
    new_two = level_two - outer_rate * (delta_two + momentum_decay * next_moment_two)
    return (new_one, new_two, next_moment_one, next_moment_two)
```

```python
import functools

import jax
import jax.numpy as jnp
from jax import lax
from jax.experimental import pallas as pl
from jax.experimental.pallas import tpu as pltpu
from jax.sharding import PartitionSpec as P

STEPS = 3


inner_rate = 64.0
outer_rate = 0.7
momentum_decay = 0.9

MESH = pl.DeviceIdType.MESH


def normalize(values):
    return values * lax.rsqrt(jnp.mean(values * values, axis=-1, keepdims=True) + 1e-06)


def path_loss(weights, inputs, targets, total):
    first, second = weights
    factor = inputs.shape[-1] ** (-0.5)
    hidden_in = (
        jnp.dot(
            normalize(inputs).astype(jnp.bfloat16),
            first.astype(jnp.bfloat16),
            preferred_element_type=jnp.float32,
        )
        * factor
    )
    hidden = inputs + jax.nn.silu(hidden_in)
    output = (
        hidden
        + jnp.dot(
            normalize(hidden).astype(jnp.bfloat16),
            second.astype(jnp.bfloat16),
            preferred_element_type=jnp.float32,
        )
        * factor
    )
    error = output - targets
    return 0.5 * jnp.sum(error * error) / total


def train_path(first, second, inputs, targets, total):
    for turn in range(STEPS):
        grads = jax.grad(path_loss)((first, second), inputs, targets, total)
        first = first - inner_rate * grads[0]
        second = second - inner_rate * grads[1]
    return (first, second)


def exchange_kernel(
    n_row, n_col, out_ref, cnt_ref, one_ref, two_ref,
    arrived, counts, whole_one, whole_two,
    doc_send, doc_recv, cnt_send, cnt_recv, up_send, down_send, one_recv,
    pair_send, pair_recv, two_send, two_recv, local_sem,
):
    row, col = lax.axis_index("row"), lax.axis_index("col")
    n = n_row * n_col
    me = row * n_col + col
    chips = n_col // 2
    place, core = col // 2, col % 2

    def device(index):
        return {"row": index // n_col, "col": index % n_col}

    barrier = pltpu.get_barrier_semaphore()

    def greet(k, carry):
        pl.semaphore_signal(
            barrier, inc=1, device_id=device((me + k) % n), device_id_type=MESH
        )
        return carry

    lax.fori_loop(1, n, greet, 0)
    own = [
        pltpu.make_async_copy(out_ref.at[me], arrived.at[me], local_sem.at[0]),
        pltpu.make_async_copy(cnt_ref.at[me], counts.at[me], local_sem.at[1]),
        pltpu.make_async_copy(one_ref, whole_one.at[col], local_sem.at[2]),
        pltpu.make_async_copy(two_ref, whole_two.at[row], local_sem.at[3]),
    ]
    for copy in own:
        copy.start()
    pl.semaphore_wait(barrier, n - 1)

    def along(source, block, to, send):
        return pltpu.make_async_remote_copy(
            src_ref=source,
            dst_ref=whole_one.at[block],
            send_sem=send.at[block],
            recv_sem=one_recv.at[block],
            device_id={"row": row, "col": to},
            device_id_type=MESH,
        )

    def across(source, block):
        return pltpu.make_async_remote_copy(
            src_ref=source,
            dst_ref=whole_one.at[block],
            send_sem=pair_send.at[block],
            recv_sem=pair_recv.at[block],
            device_id={"row": row, "col": place * 2 + 1 - core},
            device_id_type=MESH,
        )

    @pl.when(place < chips - 1)
    def _():
        along(one_ref, col, col + 2, up_send).start()

    @pl.when(place > 0)
    def _():
        along(one_ref, col, col - 2, down_send).start()

    across(one_ref, col).start()

    def two_copy(k):
        to = (row + k) % n_row
        return pltpu.make_async_remote_copy(
            src_ref=two_ref,
            dst_ref=whole_two.at[row],
            send_sem=two_send.at[k],
            recv_sem=two_recv.at[k],
            device_id={"row": to, "col": col},
            device_id_type=MESH,
        )

    def doc_copy(k):
        to = (me + k) % n
        return pltpu.make_async_remote_copy(
            src_ref=out_ref.at[to],
            dst_ref=arrived.at[me],
            send_sem=doc_send.at[k],
            recv_sem=doc_recv.at[k],
            device_id=device(to),
            device_id_type=MESH,
        )

    def cnt_copy(k):
        to = (me + k) % n
        return pltpu.make_async_remote_copy(
            src_ref=cnt_ref.at[to],
            dst_ref=counts.at[me],
            send_sem=cnt_send.at[k],
            recv_sem=cnt_recv.at[k],
            device_id=device(to),
            device_id_type=MESH,
        )

    def send_docs(low, high):
        def body(k, carry):
            doc_copy(k).start()
            cnt_copy(k).start()
            return carry

        lax.fori_loop(low, high, body, 0)

    def send_two(k, carry):
        two_copy(k).start()
        return carry

    lax.fori_loop(1, n_row, send_two, 0)
    cuts = [1 + (n - 1) * i // (chips - 1) for i in range(chips)]
    for step in range(1, chips):
        send_docs(cuts[step - 1], cuts[step])
        low, high = col - 2 * step, col + 2 * step

        @pl.when(place >= step)
        def _():
            along(one_ref, low, col, up_send).wait_recv()
            across(whole_one.at[low], low).start()

        @pl.when((place >= step) & (place < chips - 1))
        def _():
            along(whole_one.at[low], low, col + 2, up_send).start()

        @pl.when(place < chips - step)
        def _():
            along(one_ref, high, col, down_send).wait_recv()
            across(whole_one.at[high], high).start()

        @pl.when((place < chips - step) & (place > 0))
        def _():
            along(whole_one.at[high], high, col - 2, down_send).start()

    for copy in own:
        copy.wait()

    for q in range(chips):
        block = 2 * q + core
        across(one_ref, block).wait_send()
        across(one_ref, 2 * q + 1 - core).wait_recv()

        @pl.when((place >= q) & (place < chips - 1))
        def _():
            along(one_ref, block, col + 2, up_send).wait_send()

        @pl.when((place <= q) & (place > 0))
        def _():
            along(one_ref, block, col - 2, down_send).wait_send()

    def end_two(k, carry):
        two_copy(k).wait()
        return carry

    lax.fori_loop(1, n_row, end_two, 0)

    def end_docs(k, carry):
        doc_copy(k).wait()
        cnt_copy(k).wait()
        return carry

    lax.fori_loop(1, n, end_docs, 0)


def exchange(n_row, n_col, outgoing, tallies, level_one, level_two):
    n = n_row * n_col
    vmem = pl.BlockSpec(memory_space=pltpu.VMEM)
    dma = pltpu.SemaphoreType.DMA
    return pl.pallas_call(
        functools.partial(exchange_kernel, n_row, n_col),
        out_shape=(
            jax.ShapeDtypeStruct(outgoing.shape, outgoing.dtype),
            jax.ShapeDtypeStruct(tallies.shape, tallies.dtype),
            jax.ShapeDtypeStruct((n_col,) + level_one.shape, level_one.dtype),
            jax.ShapeDtypeStruct((n_row,) + level_two.shape, level_two.dtype),
        ),
        in_specs=[vmem] * 4,
        out_specs=(vmem,) * 4,
        scratch_shapes=[
            dma((n,)), dma((n,)), dma((n,)), dma((n,)),
            dma((n_col,)), dma((n_col,)), dma((n_col,)), dma((n_col,)), dma((n_col,)),
            dma((n_row,)), dma((n_row,)), dma((4,)),
        ],
        compiler_params=pltpu.CompilerParams(collective_id=0, has_side_effects=True),
    )(outgoing, tallies, level_one, level_two)


def scatter_kernel(
    n_row, n_col, one_ref, two_ref, share_one, share_two,
    pair_buf, part_buf, one_buf, two_buf,
    pair_send, pair_recv, one_send, one_recv, two_send, two_recv,
):
    row, col = lax.axis_index("row"), lax.axis_index("col")
    chips = n_col // 2
    place, core = col // 2, col % 2
    barrier = pltpu.get_barrier_semaphore()

    def greet(to_row, to_col):
        pl.semaphore_signal(
            barrier, inc=1, device_id={"row": to_row, "col": to_col}, device_id_type=MESH
        )

    partner = place * 2 + 1 - core
    greet(row, partner)
    for k in range(1, chips):
        greet(row, (col + 2 * k) % n_col)
    for k in range(1, n_row):
        greet((row + k) % n_row, col)
    pl.semaphore_wait(barrier, chips + n_row - 1)

    def pair_copy(q):
        return pltpu.make_async_remote_copy(
            src_ref=one_ref.at[2 * q + 1 - core],
            dst_ref=pair_buf.at[q],
            send_sem=pair_send.at[q],
            recv_sem=pair_recv.at[q],
            device_id={"row": row, "col": partner},
            device_id_type=MESH,
        )

    def two_copy(k):
        to = (row + k) % n_row
        return pltpu.make_async_remote_copy(
            src_ref=two_ref.at[to],
            dst_ref=two_buf.at[k],
            send_sem=two_send.at[k],
            recv_sem=two_recv.at[k],
            device_id={"row": to, "col": col},
            device_id_type=MESH,
        )

    def one_copy(k):
        return pltpu.make_async_remote_copy(
            src_ref=part_buf.at[k],
            dst_ref=one_buf.at[k],
            send_sem=one_send.at[k],
            recv_sem=one_recv.at[k],
            device_id={"row": row, "col": (col + 2 * k) % n_col},
            device_id_type=MESH,
        )

    for k in range(1, chips):
        pair_copy((place + k) % chips).start()
    pair_copy(place).start()
    for k in range(1, n_row):
        two_copy(k).start()
    for k in range(1, chips):
        q = (place + k) % chips
        pair_copy(q).wait_recv()
        part_buf[k] = (
            one_ref[2 * q + core].astype(jnp.float32) + pair_buf[q].astype(jnp.float32)
        ).astype(jnp.bfloat16)
        one_copy(k).start()
    pair_copy(place).wait_recv()
    share_one[...] = one_ref[col].astype(jnp.float32) + pair_buf[place].astype(jnp.float32)
    share_two[...] = two_ref[row].astype(jnp.float32)
    for k in range(1, chips):
        one_copy(k).wait_recv()
        share_one[...] += one_buf[k].astype(jnp.float32)
    for k in range(1, n_row):
        two_copy(k).wait_recv()
        share_two[...] += two_buf[k].astype(jnp.float32)
    for q in range(chips):
        pair_copy(q).wait_send()
    for k in range(1, chips):
        one_copy(k).wait_send()
    for k in range(1, n_row):
        two_copy(k).wait_send()


def scatter(n_row, n_col, change_one, change_two):
    width = change_one.shape[-1]
    chips = n_col // 2
    rows_one, rows_two = width // n_col, width // n_row
    vmem = pl.BlockSpec(memory_space=pltpu.VMEM)
    dma = pltpu.SemaphoreType.DMA
    return pl.pallas_call(
        functools.partial(scatter_kernel, n_row, n_col),
        out_shape=(
            jax.ShapeDtypeStruct((rows_one, width), jnp.float32),
            jax.ShapeDtypeStruct((rows_two, width), jnp.float32),
        ),
        in_specs=[vmem] * 2,
        out_specs=(vmem,) * 2,
        scratch_shapes=[
            pltpu.VMEM((chips, rows_one, width), jnp.bfloat16),
            pltpu.VMEM((chips, rows_one, width), jnp.bfloat16),
            pltpu.VMEM((chips, rows_one, width), jnp.bfloat16),
            pltpu.VMEM((n_row, rows_two, width), jnp.bfloat16),
            dma((chips,)), dma((chips,)), dma((chips,)), dma((chips,)),
            dma((n_row,)), dma((n_row,)),
        ],
        compiler_params=pltpu.CompilerParams(collective_id=1, has_side_effects=True),
    )(
        change_one.reshape(n_col, rows_one, width),
        change_two.reshape(n_row, rows_two, width),
    )


def shards(docs, routes, level_one, level_two, moment_one, moment_two):
    n_row = lax.axis_size("row")
    n_col = lax.axis_size("col")
    paths = n_row * n_col
    count = docs.shape[0]
    length = docs.shape[1]
    width = docs.shape[2]
    capacity = max(2, (2 * count + paths - 1) // paths)
    target = routes[:, 0]
    places = jnp.arange(count, dtype=jnp.int32)
    same = (target[:, None] == target[None, :]) & (places[None, :] < places[:, None])
    rank = jnp.sum(same.astype(jnp.int32), axis=1)
    steps = jnp.arange(length, dtype=jnp.int32)
    line = ((target * length * capacity + rank)[:, None] + steps[None, :] * capacity).reshape(-1)
    dispatch = (
        jnp.arange(paths * length * capacity, dtype=jnp.int32)[:, None] == line[None, :]
    ).astype(jnp.bfloat16)
    outgoing = jnp.dot(
        dispatch, docs.reshape(count * length, width), preferred_element_type=jnp.float32
    ).astype(jnp.bfloat16)
    tally = jnp.sum(
        (target[None, :] == jnp.arange(paths, dtype=jnp.int32)[:, None]).astype(jnp.float32), axis=1
    )
    tallies = jnp.broadcast_to(tally[:, None, None], (paths, 8, 128))
    arrived, counts, whole_one, whole_two = exchange(
        n_row,
        n_col,
        outgoing.reshape(paths, length * capacity, width),
        tallies,
        level_one[0].astype(jnp.bfloat16),
        level_two[0].astype(jnp.bfloat16),
    )
    total = jnp.sum(counts[:, 0, 0]) * (length - 1)
    blocks = arrived.astype(jnp.float32)
    inputs = blocks[:, : (length - 1) * capacity].reshape(-1, width)
    targets = blocks[:, capacity:].reshape(-1, width)
    whole_one = whole_one.reshape(width, width).astype(jnp.float32)
    whole_two = whole_two.reshape(width, width).astype(jnp.float32)
    end_one, end_two = train_path(whole_one, whole_two, inputs, targets, total)
    share_one, share_two = scatter(
        n_row,
        n_col,
        (whole_one - end_one).astype(jnp.bfloat16),
        (whole_two - end_two).astype(jnp.bfloat16),
    )
    delta_one = (share_one / n_col)[None]
    delta_two = (share_two / n_row)[None]
    next_moment_one = momentum_decay * moment_one + delta_one
    next_moment_two = momentum_decay * moment_two + delta_two
    new_one = level_one - outer_rate * (delta_one + momentum_decay * next_moment_one)
    new_two = level_two - outer_rate * (delta_two + momentum_decay * next_moment_two)
    return (new_one, new_two, next_moment_one, next_moment_two)


def solution(mesh):
    placed = (
        P(("row", "col"), None, None),
        P(("row", "col"), None),
        P("row", "col", None),
        P("col", "row", None),
        P("row", "col", None),
        P("col", "row", None),
    )
    return jax.shard_map(
        shards,
        mesh=mesh,
        in_specs=placed,
        out_specs=(
            P("row", "col", None),
            P("col", "row", None),
            P("row", "col", None),
            P("col", "row", None),
        ),
        check_vma=False,
    )
```

```python
import functools

import jax
import jax.numpy as jnp
from jax import lax
from jax.experimental import pallas as pl
from jax.experimental.pallas import tpu as pltpu
from jax.sharding import PartitionSpec as P

STEPS = 3


inner_rate = 64.0
outer_rate = 0.7
momentum_decay = 0.9

MESH = pl.DeviceIdType.MESH


def normalize(values):
    return values * lax.rsqrt(jnp.mean(values * values, axis=-1, keepdims=True) + 1e-06)


def path_loss(weights, inputs, targets, total):
    first, second = weights
    factor = inputs.shape[-1] ** (-0.5)
    hidden_in = (
        jnp.dot(
            normalize(inputs).astype(jnp.bfloat16),
            first.astype(jnp.bfloat16),
            preferred_element_type=jnp.float32,
        )
        * factor
    )
    hidden = inputs + jax.nn.silu(hidden_in)
    output = (
        hidden
        + jnp.dot(
            normalize(hidden).astype(jnp.bfloat16),
            second.astype(jnp.bfloat16),
            preferred_element_type=jnp.float32,
        )
        * factor
    )
    error = output - targets
    return 0.5 * jnp.sum(error * error) / total


def train_path(first, second, inputs, targets, total):
    for turn in range(STEPS):
        grads = jax.grad(path_loss)((first, second), inputs, targets, total)
        first = first - inner_rate * grads[0]
        second = second - inner_rate * grads[1]
    return (first, second)


def exchange_kernel(
    n_row, n_col, line_ref, docs_ref, level_one_ref, level_two_ref,
    arrived, counts, whole_one, whole_two,
    out_ref, cnt_ref, one_ref, two_ref,
    doc_send, doc_recv, cnt_send, cnt_recv, up_send, down_send, one_recv,
    pair_send, pair_recv, two_send, two_recv, local_sem,
):
    row, col = lax.axis_index("row"), lax.axis_index("col")
    n = n_row * n_col
    me = row * n_col + col
    chips = n_col // 2
    place, core = col // 2, col % 2
    lines, width = arrived.shape[1:]
    depth = docs_ref.shape[0]
    barrier = pltpu.get_barrier_semaphore()

    def greet(k, carry):
        to = (me + k) % n
        pl.semaphore_signal(
            barrier, inc=1, device_id={"row": to // n_col, "col": to % n_col}, device_id_type=MESH
        )
        return carry

    lax.fori_loop(1, n, greet, 0)
    one_ref[...] = level_one_ref[...].astype(jnp.bfloat16)
    two_ref[...] = level_two_ref[...].astype(jnp.bfloat16)
    pl.semaphore_wait(barrier, n - 1)

    def along(source, block, to, send):
        return pltpu.make_async_remote_copy(
            src_ref=source,
            dst_ref=whole_one.at[block],
            send_sem=send.at[block],
            recv_sem=one_recv.at[block],
            device_id={"row": row, "col": to},
            device_id_type=MESH,
        )

    def across(source, block):
        return pltpu.make_async_remote_copy(
            src_ref=source,
            dst_ref=whole_one.at[block],
            send_sem=pair_send.at[block],
            recv_sem=pair_recv.at[block],
            device_id={"row": row, "col": place * 2 + 1 - core},
            device_id_type=MESH,
        )

    @pl.when(place < chips - 1)
    def _():
        along(one_ref, col, col + 2, up_send).start()

    @pl.when(place > 0)
    def _():
        along(one_ref, col, col - 2, down_send).start()

    across(one_ref, col).start()

    def two_copy(k):
        to = (row + k) % n_row
        return pltpu.make_async_remote_copy(
            src_ref=two_ref,
            dst_ref=whole_two.at[row],
            send_sem=two_send.at[k],
            recv_sem=two_recv.at[k],
            device_id={"row": to, "col": col},
            device_id_type=MESH,
        )

    for k in range(1, n_row):
        two_copy(k).start()

    own = [
        pltpu.make_async_copy(one_ref, whole_one.at[col], local_sem.at[0]),
        pltpu.make_async_copy(two_ref, whole_two.at[row], local_sem.at[1]),
        pltpu.make_async_copy(out_ref.at[me], arrived.at[me], local_sem.at[2]),
        pltpu.make_async_copy(cnt_ref.at[me], counts.at[me], local_sem.at[3]),
    ]
    own[0].start()
    own[1].start()

    path = lax.broadcasted_iota(jnp.int32, (n, 8, depth), 0) * lines
    wide = jnp.broadcast_to(line_ref[...][None], (n, 8, depth))
    named = ((wide >= path) & (wide < path + lines)).astype(jnp.float32)
    cnt_ref[...] = jnp.broadcast_to(jnp.sum(named, axis=-1, keepdims=True), cnt_ref.shape)

    def pair_of(shift, turn):
        to_row, to_col = (row + shift) % n_row, (col + turn) % n_col
        to = to_row * n_col + to_col
        k = shift * n_col + turn
        peer = {"row": to_row, "col": to_col}
        return (
            pltpu.make_async_remote_copy(
                src_ref=out_ref.at[to],
                dst_ref=arrived.at[me],
                send_sem=doc_send.at[k],
                recv_sem=doc_recv.at[k],
                device_id=peer,
                device_id_type=MESH,
            ),
            pltpu.make_async_remote_copy(
                src_ref=cnt_ref.at[to],
                dst_ref=counts.at[me],
                send_sem=cnt_send.at[k],
                recv_sem=cnt_recv.at[k],
                device_id=peer,
                device_id_type=MESH,
            ),
        )

    def send_group(shift):
        to_row = (row + shift) % n_row
        base = to_row * n_col * lines
        index = lax.broadcasted_iota(jnp.int32, (n_col * lines, depth), 0) + base
        dispatch = (index == line_ref[...]).astype(jnp.float32).astype(jnp.bfloat16)
        rows = jnp.dot(dispatch, docs_ref[...], preferred_element_type=jnp.float32)
        out_ref[pl.ds(to_row * n_col, n_col)] = rows.reshape(n_col, lines, width).astype(
            jnp.bfloat16
        )

        def body(turn, carry):
            for copy in pair_of(shift, turn):
                copy.start()
            return carry

        lax.fori_loop(1 if shift == 0 else 0, n_col, body, 0)
        if shift == 0:
            own[2].start()
            own[3].start()

    for step in range(1, max(n_row, chips - 1) + 1):
        if step <= n_row:
            send_group(step % n_row)
        if step < chips:
            low, high = col - 2 * step, col + 2 * step

            @pl.when(place >= step)
            def _():
                along(one_ref, low, col, up_send).wait_recv()
                across(whole_one.at[low], low).start()

            @pl.when((place >= step) & (place < chips - 1))
            def _():
                along(whole_one.at[low], low, col + 2, up_send).start()

            @pl.when(place < chips - step)
            def _():
                along(one_ref, high, col, down_send).wait_recv()
                across(whole_one.at[high], high).start()

            @pl.when((place < chips - step) & (place > 0))
            def _():
                along(whole_one.at[high], high, col - 2, down_send).start()

    for copy in own:
        copy.wait()

    for q in range(chips):
        block = 2 * q + core
        across(one_ref, block).wait_send()
        across(one_ref, 2 * q + 1 - core).wait_recv()

        @pl.when((place >= q) & (place < chips - 1))
        def _():
            along(one_ref, block, col + 2, up_send).wait_send()

        @pl.when((place <= q) & (place > 0))
        def _():
            along(one_ref, block, col - 2, down_send).wait_send()

    for k in range(1, n_row):
        two_copy(k).wait()

    for shift in range(n_row):

        def finish(turn, carry):
            for copy in pair_of(shift, turn):
                copy.wait()
            return carry

        lax.fori_loop(1 if shift == 0 else 0, n_col, finish, 0)


def exchange(n_row, n_col, lines, line, docs, level_one, level_two):
    n = n_row * n_col
    width = docs.shape[-1]
    vmem = pl.BlockSpec(memory_space=pltpu.VMEM)
    dma = pltpu.SemaphoreType.DMA
    return pl.pallas_call(
        functools.partial(exchange_kernel, n_row, n_col),
        out_shape=(
            jax.ShapeDtypeStruct((n, lines, width), jnp.bfloat16),
            jax.ShapeDtypeStruct((n, 8, 128), jnp.float32),
            jax.ShapeDtypeStruct((n_col,) + level_one.shape, jnp.bfloat16),
            jax.ShapeDtypeStruct((n_row,) + level_two.shape, jnp.bfloat16),
        ),
        in_specs=[vmem] * 4,
        out_specs=(vmem,) * 4,
        scratch_shapes=[
            pltpu.VMEM((n, lines, width), jnp.bfloat16),
            pltpu.VMEM((n, 8, 128), jnp.float32),
            pltpu.VMEM(level_one.shape, jnp.bfloat16),
            pltpu.VMEM(level_two.shape, jnp.bfloat16),
            dma((n,)), dma((n,)), dma((n,)), dma((n,)),
            dma((n_col,)), dma((n_col,)), dma((n_col,)), dma((n_col,)), dma((n_col,)),
            dma((n_row,)), dma((n_row,)), dma((4,)),
        ],
        compiler_params=pltpu.CompilerParams(collective_id=0, has_side_effects=True),
    )(line, docs, level_one, level_two)


def scatter_kernel(
    n_row, n_col, one_ref, two_ref, share_one, share_two,
    pair_buf, part_buf, one_buf, two_buf,
    pair_send, pair_recv, one_send, one_recv, two_send, two_recv,
):
    row, col = lax.axis_index("row"), lax.axis_index("col")
    chips = n_col // 2
    place, core = col // 2, col % 2
    barrier = pltpu.get_barrier_semaphore()

    def greet(to_row, to_col):
        pl.semaphore_signal(
            barrier, inc=1, device_id={"row": to_row, "col": to_col}, device_id_type=MESH
        )

    partner = place * 2 + 1 - core
    greet(row, partner)
    for k in range(1, chips):
        greet(row, (col + 2 * k) % n_col)
    for k in range(1, n_row):
        greet((row + k) % n_row, col)
    pl.semaphore_wait(barrier, chips + n_row - 1)

    def pair_copy(q):
        return pltpu.make_async_remote_copy(
            src_ref=one_ref.at[2 * q + 1 - core],
            dst_ref=pair_buf.at[q],
            send_sem=pair_send.at[q],
            recv_sem=pair_recv.at[q],
            device_id={"row": row, "col": partner},
            device_id_type=MESH,
        )

    def two_copy(k):
        to = (row + k) % n_row
        return pltpu.make_async_remote_copy(
            src_ref=two_ref.at[to],
            dst_ref=two_buf.at[k],
            send_sem=two_send.at[k],
            recv_sem=two_recv.at[k],
            device_id={"row": to, "col": col},
            device_id_type=MESH,
        )

    def one_copy(k):
        return pltpu.make_async_remote_copy(
            src_ref=part_buf.at[k],
            dst_ref=one_buf.at[k],
            send_sem=one_send.at[k],
            recv_sem=one_recv.at[k],
            device_id={"row": row, "col": (col + 2 * k) % n_col},
            device_id_type=MESH,
        )

    for k in range(1, chips):
        pair_copy((place + k) % chips).start()
    pair_copy(place).start()
    for k in range(1, n_row):
        two_copy(k).start()
    for k in range(1, chips):
        q = (place + k) % chips
        pair_copy(q).wait_recv()
        part_buf[k] = (
            one_ref[2 * q + core].astype(jnp.float32) + pair_buf[q].astype(jnp.float32)
        ).astype(jnp.bfloat16)
        one_copy(k).start()
    pair_copy(place).wait_recv()
    share_one[...] = one_ref[col].astype(jnp.float32) + pair_buf[place].astype(jnp.float32)
    share_two[...] = two_ref[row].astype(jnp.float32)
    for k in range(1, chips):
        one_copy(k).wait_recv()
        share_one[...] += one_buf[k].astype(jnp.float32)
    for k in range(1, n_row):
        two_copy(k).wait_recv()
        share_two[...] += two_buf[k].astype(jnp.float32)
    for q in range(chips):
        pair_copy(q).wait_send()
    for k in range(1, chips):
        one_copy(k).wait_send()
    for k in range(1, n_row):
        two_copy(k).wait_send()


def scatter(n_row, n_col, change_one, change_two):
    width = change_one.shape[-1]
    chips = n_col // 2
    rows_one, rows_two = width // n_col, width // n_row
    vmem = pl.BlockSpec(memory_space=pltpu.VMEM)
    dma = pltpu.SemaphoreType.DMA
    return pl.pallas_call(
        functools.partial(scatter_kernel, n_row, n_col),
        out_shape=(
            jax.ShapeDtypeStruct((rows_one, width), jnp.float32),
            jax.ShapeDtypeStruct((rows_two, width), jnp.float32),
        ),
        in_specs=[vmem] * 2,
        out_specs=(vmem,) * 2,
        scratch_shapes=[
            pltpu.VMEM((chips, rows_one, width), jnp.bfloat16),
            pltpu.VMEM((chips, rows_one, width), jnp.bfloat16),
            pltpu.VMEM((chips, rows_one, width), jnp.bfloat16),
            pltpu.VMEM((n_row, rows_two, width), jnp.bfloat16),
            dma((chips,)), dma((chips,)), dma((chips,)), dma((chips,)),
            dma((n_row,)), dma((n_row,)),
        ],
        compiler_params=pltpu.CompilerParams(collective_id=1, has_side_effects=True),
    )(
        change_one.reshape(n_col, rows_one, width),
        change_two.reshape(n_row, rows_two, width),
    )


def shards(docs, routes, level_one, level_two, moment_one, moment_two):
    n_row = lax.axis_size("row")
    n_col = lax.axis_size("col")
    paths = n_row * n_col
    count = docs.shape[0]
    length = docs.shape[1]
    width = docs.shape[2]
    capacity = max(2, (2 * count + paths - 1) // paths)
    target = routes[:, 0]
    places = jnp.arange(count, dtype=jnp.int32)
    same = (target[:, None] == target[None, :]) & (places[None, :] < places[:, None])
    rank = jnp.sum(same.astype(jnp.int32), axis=1)
    steps = jnp.arange(length, dtype=jnp.int32)
    line = ((target * length * capacity + rank)[:, None] + steps[None, :] * capacity).reshape(-1)
    arrived, counts, whole_one, whole_two = exchange(
        n_row,
        n_col,
        length * capacity,
        line[None, :],
        docs.reshape(count * length, width),
        level_one[0],
        level_two[0],
    )
    total = jnp.sum(counts[:, 0, 0]) * ((length - 1) / length)
    blocks = arrived.astype(jnp.float32)
    inputs = blocks[:, : (length - 1) * capacity].reshape(-1, width)
    targets = blocks[:, capacity:].reshape(-1, width)
    whole_one = whole_one.reshape(width, width).astype(jnp.float32)
    whole_two = whole_two.reshape(width, width).astype(jnp.float32)
    end_one, end_two = train_path(whole_one, whole_two, inputs, targets, total)
    share_one, share_two = scatter(
        n_row,
        n_col,
        (whole_one - end_one).astype(jnp.bfloat16),
        (whole_two - end_two).astype(jnp.bfloat16),
    )
    delta_one = (share_one / n_col)[None]
    delta_two = (share_two / n_row)[None]
    next_moment_one = momentum_decay * moment_one + delta_one
    next_moment_two = momentum_decay * moment_two + delta_two
    new_one = level_one - outer_rate * (delta_one + momentum_decay * next_moment_one)
    new_two = level_two - outer_rate * (delta_two + momentum_decay * next_moment_two)
    return (new_one, new_two, next_moment_one, next_moment_two)


def solution(mesh):
    placed = (
        P(("row", "col"), None, None),
        P(("row", "col"), None),
        P("row", "col", None),
        P("col", "row", None),
        P("row", "col", None),
        P("col", "row", None),
    )
    return jax.shard_map(
        shards,
        mesh=mesh,
        in_specs=placed,
        out_specs=(
            P("row", "col", None),
            P("col", "row", None),
            P("row", "col", None),
            P("col", "row", None),
        ),
        check_vma=False,
    )
```

```python
import functools

import jax
import jax.numpy as jnp
from jax import lax
from jax.experimental import pallas as pl
from jax.experimental.pallas import tpu as pltpu
from jax.sharding import PartitionSpec as P

STEPS = 3


inner_rate = 64.0
outer_rate = 0.7
momentum_decay = 0.9

MESH = pl.DeviceIdType.MESH


def normalize(values):
    return values * lax.rsqrt(jnp.mean(values * values, axis=-1, keepdims=True) + 1e-06)


def path_loss(weights, inputs, targets, total):
    first, second = weights
    factor = inputs.shape[-1] ** (-0.5)
    hidden_in = (
        jnp.dot(
            normalize(inputs).astype(jnp.bfloat16),
            first.astype(jnp.bfloat16),
            preferred_element_type=jnp.float32,
        )
        * factor
    )
    hidden = inputs + jax.nn.silu(hidden_in)
    output = (
        hidden
        + jnp.dot(
            normalize(hidden).astype(jnp.bfloat16),
            second.astype(jnp.bfloat16),
            preferred_element_type=jnp.float32,
        )
        * factor
    )
    error = output - targets
    return 0.5 * jnp.sum(error * error) / total


def train_path(first, second, inputs, targets, total):
    for turn in range(STEPS):
        grads = jax.grad(path_loss)((first, second), inputs, targets, total)
        first = first - inner_rate * grads[0]
        second = second - inner_rate * grads[1]
    return (first, second)


def exchange_kernel(
    n_row, n_col, line_ref, docs_ref, level_one_ref, level_two_ref,
    inputs, targets, total, whole_one, whole_two,
    arrived, counts, out_ref, cnt_ref, one_ref, two_ref,
    doc_send, doc_recv, cnt_send, cnt_recv, up_send, down_send, one_recv,
    pair_send, pair_recv, two_send, two_recv, local_sem,
):
    row, col = lax.axis_index("row"), lax.axis_index("col")
    n = n_row * n_col
    me = row * n_col + col
    chips = n_col // 2
    place, core = col // 2, col % 2
    lines, width = arrived.shape[1:]
    kept = inputs.shape[1]
    depth = docs_ref.shape[0]
    barrier = pltpu.get_barrier_semaphore()

    def greet(k, carry):
        to = (me + k) % n
        pl.semaphore_signal(
            barrier, inc=1, device_id={"row": to // n_col, "col": to % n_col}, device_id_type=MESH
        )
        return carry

    lax.fori_loop(1, n, greet, 0)
    one_ref[...] = level_one_ref[...].astype(jnp.bfloat16)
    two_ref[...] = level_two_ref[...].astype(jnp.bfloat16)
    pl.semaphore_wait(barrier, n - 1)

    def along(source, block, to, send):
        return pltpu.make_async_remote_copy(
            src_ref=source,
            dst_ref=whole_one.at[block],
            send_sem=send.at[block],
            recv_sem=one_recv.at[block],
            device_id={"row": row, "col": to},
            device_id_type=MESH,
        )

    def across(source, block):
        return pltpu.make_async_remote_copy(
            src_ref=source,
            dst_ref=whole_one.at[block],
            send_sem=pair_send.at[block],
            recv_sem=pair_recv.at[block],
            device_id={"row": row, "col": place * 2 + 1 - core},
            device_id_type=MESH,
        )

    @pl.when(place < chips - 1)
    def _():
        along(one_ref, col, col + 2, up_send).start()

    @pl.when(place > 0)
    def _():
        along(one_ref, col, col - 2, down_send).start()

    across(one_ref, col).start()

    def two_copy(k):
        to = (row + k) % n_row
        return pltpu.make_async_remote_copy(
            src_ref=two_ref,
            dst_ref=whole_two.at[row],
            send_sem=two_send.at[k],
            recv_sem=two_recv.at[k],
            device_id={"row": to, "col": col},
            device_id_type=MESH,
        )

    for k in range(1, n_row):
        two_copy(k).start()

    own = [
        pltpu.make_async_copy(one_ref, whole_one.at[col], local_sem.at[0]),
        pltpu.make_async_copy(two_ref, whole_two.at[row], local_sem.at[1]),
        pltpu.make_async_copy(out_ref.at[me], arrived.at[me], local_sem.at[2]),
        pltpu.make_async_copy(cnt_ref.at[me], counts.at[me], local_sem.at[3]),
    ]
    own[0].start()
    own[1].start()

    path = lax.broadcasted_iota(jnp.int32, (n, 1, depth), 0) * lines
    wide = jnp.broadcast_to(line_ref[...][None], (n, 1, depth))
    named = ((wide >= path) & (wide < path + lines)).astype(jnp.float32)
    cnt_ref[...] = jnp.broadcast_to(jnp.sum(named, axis=-1, keepdims=True), cnt_ref.shape)

    def pair_of(shift, turn):
        to_row, to_col = (row + shift) % n_row, (col + turn) % n_col
        to = to_row * n_col + to_col
        k = shift * n_col + turn
        peer = {"row": to_row, "col": to_col}
        return (
            pltpu.make_async_remote_copy(
                src_ref=out_ref.at[to],
                dst_ref=arrived.at[me],
                send_sem=doc_send.at[k],
                recv_sem=doc_recv.at[k],
                device_id=peer,
                device_id_type=MESH,
            ),
            pltpu.make_async_remote_copy(
                src_ref=cnt_ref.at[to],
                dst_ref=counts.at[me],
                send_sem=cnt_send.at[k],
                recv_sem=cnt_recv.at[k],
                device_id=peer,
                device_id_type=MESH,
            ),
        )

    def send_group(shift):
        to_row = (row + shift) % n_row
        base = to_row * n_col * lines
        index = lax.broadcasted_iota(jnp.int32, (n_col * lines, depth), 0) + base
        dispatch = (index == line_ref[...]).astype(jnp.float32).astype(jnp.bfloat16)
        rows = jnp.dot(dispatch, docs_ref[...], preferred_element_type=jnp.float32)
        out_ref[pl.ds(to_row * n_col, n_col)] = rows.reshape(n_col, lines, width).astype(
            jnp.bfloat16
        )

        def body(turn, carry):
            for copy in pair_of(shift, turn):
                copy.start()
            return carry

        lax.fori_loop(1 if shift == 0 else 0, n_col, body, 0)
        if shift == 0:
            own[2].start()
            own[3].start()

    for step in range(1, max(n_row, chips - 1) + 1):
        if step <= n_row:
            send_group(step % n_row)
        if step < chips:
            low, high = col - 2 * step, col + 2 * step

            @pl.when(place >= step)
            def _():
                along(one_ref, low, col, up_send).wait_recv()
                across(whole_one.at[low], low).start()

            @pl.when((place >= step) & (place < chips - 1))
            def _():
                along(whole_one.at[low], low, col + 2, up_send).start()

            @pl.when(place < chips - step)
            def _():
                along(one_ref, high, col, down_send).wait_recv()
                across(whole_one.at[high], high).start()

            @pl.when((place < chips - step) & (place > 0))
            def _():
                along(whole_one.at[high], high, col - 2, down_send).start()

    def unpack(source):
        rows = arrived[source].astype(jnp.float32)
        inputs[source] = rows[:kept]
        targets[source] = rows[lines - kept :]
        total[...] += counts[source]

    for copy in own:
        copy.wait()
    total[...] = jnp.zeros_like(total)
    unpack(me)

    for step in range(1, n_row + 1):
        shift = step % n_row

        def finish(turn, carry):
            for copy in pair_of(shift, turn):
                copy.wait()
            unpack((row - shift + n_row) % n_row * n_col + (col - turn + n_col) % n_col)
            return carry

        lax.fori_loop(1 if shift == 0 else 0, n_col, finish, 0)

    for q in range(chips):
        block = 2 * q + core
        across(one_ref, block).wait_send()
        across(one_ref, 2 * q + 1 - core).wait_recv()

        @pl.when((place >= q) & (place < chips - 1))
        def _():
            along(one_ref, block, col + 2, up_send).wait_send()

        @pl.when((place <= q) & (place > 0))
        def _():
            along(one_ref, block, col - 2, down_send).wait_send()

    for k in range(1, n_row):
        two_copy(k).wait()


def exchange(n_row, n_col, lines, kept, line, docs, level_one, level_two):
    n = n_row * n_col
    width = docs.shape[-1]
    vmem = pl.BlockSpec(memory_space=pltpu.VMEM)
    dma = pltpu.SemaphoreType.DMA
    return pl.pallas_call(
        functools.partial(exchange_kernel, n_row, n_col),
        out_shape=(
            jax.ShapeDtypeStruct((n, kept, width), jnp.float32),
            jax.ShapeDtypeStruct((n, kept, width), jnp.float32),
            jax.ShapeDtypeStruct((1, 128), jnp.float32),
            jax.ShapeDtypeStruct((n_col,) + level_one.shape, jnp.bfloat16),
            jax.ShapeDtypeStruct((n_row,) + level_two.shape, jnp.bfloat16),
        ),
        in_specs=[vmem] * 4,
        out_specs=(vmem,) * 5,
        scratch_shapes=[
            pltpu.VMEM((n, lines, width), jnp.bfloat16),
            pltpu.VMEM((n, 1, 128), jnp.float32),
            pltpu.VMEM((n, lines, width), jnp.bfloat16),
            pltpu.VMEM((n, 1, 128), jnp.float32),
            pltpu.VMEM(level_one.shape, jnp.bfloat16),
            pltpu.VMEM(level_two.shape, jnp.bfloat16),
            dma((n,)), dma((n,)), dma((n,)), dma((n,)),
            dma((n_col,)), dma((n_col,)), dma((n_col,)), dma((n_col,)), dma((n_col,)),
            dma((n_row,)), dma((n_row,)), dma((4,)),
        ],
        compiler_params=pltpu.CompilerParams(collective_id=0, has_side_effects=True),
    )(line, docs, level_one, level_two)


def scatter_kernel(
    n_row, n_col, one_ref, two_ref, share_one, share_two,
    pair_buf, part_buf, one_buf, two_buf,
    pair_send, pair_recv, one_send, one_recv, two_send, two_recv,
):
    row, col = lax.axis_index("row"), lax.axis_index("col")
    chips = n_col // 2
    place, core = col // 2, col % 2
    barrier = pltpu.get_barrier_semaphore()

    def greet(to_row, to_col):
        pl.semaphore_signal(
            barrier, inc=1, device_id={"row": to_row, "col": to_col}, device_id_type=MESH
        )

    partner = place * 2 + 1 - core
    greet(row, partner)
    for k in range(1, chips):
        greet(row, (col + 2 * k) % n_col)
    for k in range(1, n_row):
        greet((row + k) % n_row, col)
    pl.semaphore_wait(barrier, chips + n_row - 1)

    def pair_copy(q):
        return pltpu.make_async_remote_copy(
            src_ref=one_ref.at[2 * q + 1 - core],
            dst_ref=pair_buf.at[q],
            send_sem=pair_send.at[q],
            recv_sem=pair_recv.at[q],
            device_id={"row": row, "col": partner},
            device_id_type=MESH,
        )

    def two_copy(k):
        to = (row + k) % n_row
        return pltpu.make_async_remote_copy(
            src_ref=two_ref.at[to],
            dst_ref=two_buf.at[k],
            send_sem=two_send.at[k],
            recv_sem=two_recv.at[k],
            device_id={"row": to, "col": col},
            device_id_type=MESH,
        )

    def one_copy(k):
        return pltpu.make_async_remote_copy(
            src_ref=part_buf.at[k],
            dst_ref=one_buf.at[k],
            send_sem=one_send.at[k],
            recv_sem=one_recv.at[k],
            device_id={"row": row, "col": (col + 2 * k) % n_col},
            device_id_type=MESH,
        )

    for k in range(1, chips):
        pair_copy((place + k) % chips).start()
    pair_copy(place).start()
    for k in range(1, n_row):
        two_copy(k).start()
    for k in range(1, chips):
        q = (place + k) % chips
        pair_copy(q).wait_recv()
        part_buf[k] = (
            one_ref[2 * q + core].astype(jnp.float32) + pair_buf[q].astype(jnp.float32)
        ).astype(jnp.bfloat16)
        one_copy(k).start()
    pair_copy(place).wait_recv()
    share_one[...] = one_ref[col].astype(jnp.float32) + pair_buf[place].astype(jnp.float32)
    share_two[...] = two_ref[row].astype(jnp.float32)
    for k in range(1, chips):
        one_copy(k).wait_recv()
        share_one[...] += one_buf[k].astype(jnp.float32)
    for k in range(1, n_row):
        two_copy(k).wait_recv()
        share_two[...] += two_buf[k].astype(jnp.float32)
    for q in range(chips):
        pair_copy(q).wait_send()
    for k in range(1, chips):
        one_copy(k).wait_send()
    for k in range(1, n_row):
        two_copy(k).wait_send()


def scatter(n_row, n_col, change_one, change_two):
    width = change_one.shape[-1]
    chips = n_col // 2
    rows_one, rows_two = width // n_col, width // n_row
    vmem = pl.BlockSpec(memory_space=pltpu.VMEM)
    dma = pltpu.SemaphoreType.DMA
    return pl.pallas_call(
        functools.partial(scatter_kernel, n_row, n_col),
        out_shape=(
            jax.ShapeDtypeStruct((rows_one, width), jnp.float32),
            jax.ShapeDtypeStruct((rows_two, width), jnp.float32),
        ),
        in_specs=[vmem] * 2,
        out_specs=(vmem,) * 2,
        scratch_shapes=[
            pltpu.VMEM((chips, rows_one, width), jnp.bfloat16),
            pltpu.VMEM((chips, rows_one, width), jnp.bfloat16),
            pltpu.VMEM((chips, rows_one, width), jnp.bfloat16),
            pltpu.VMEM((n_row, rows_two, width), jnp.bfloat16),
            dma((chips,)), dma((chips,)), dma((chips,)), dma((chips,)),
            dma((n_row,)), dma((n_row,)),
        ],
        compiler_params=pltpu.CompilerParams(collective_id=1, has_side_effects=True),
    )(
        change_one.reshape(n_col, rows_one, width),
        change_two.reshape(n_row, rows_two, width),
    )


def shards(docs, routes, level_one, level_two, moment_one, moment_two):
    n_row = lax.axis_size("row")
    n_col = lax.axis_size("col")
    paths = n_row * n_col
    count = docs.shape[0]
    length = docs.shape[1]
    width = docs.shape[2]
    capacity = max(2, (2 * count + paths - 1) // paths)
    target = routes[:, 0]
    places = jnp.arange(count, dtype=jnp.int32)
    same = (target[:, None] == target[None, :]) & (places[None, :] < places[:, None])
    rank = jnp.sum(same.astype(jnp.int32), axis=1)
    steps = jnp.arange(length, dtype=jnp.int32)
    line = ((target * length * capacity + rank)[:, None] + steps[None, :] * capacity).reshape(-1)
    inputs, targets, filled, whole_one, whole_two = exchange(
        n_row,
        n_col,
        length * capacity,
        (length - 1) * capacity,
        line[None, :],
        docs.reshape(count * length, width),
        level_one[0],
        level_two[0],
    )
    total = filled[0, 0] * ((length - 1) / length)
    inputs = inputs.reshape(-1, width)
    targets = targets.reshape(-1, width)
    whole_one = whole_one.reshape(width, width).astype(jnp.float32)
    whole_two = whole_two.reshape(width, width).astype(jnp.float32)
    end_one, end_two = train_path(whole_one, whole_two, inputs, targets, total)
    share_one, share_two = scatter(
        n_row,
        n_col,
        (whole_one - end_one).astype(jnp.bfloat16),
        (whole_two - end_two).astype(jnp.bfloat16),
    )
    delta_one = (share_one / n_col)[None]
    delta_two = (share_two / n_row)[None]
    next_moment_one = momentum_decay * moment_one + delta_one
    next_moment_two = momentum_decay * moment_two + delta_two
    new_one = level_one - outer_rate * (delta_one + momentum_decay * next_moment_one)
    new_two = level_two - outer_rate * (delta_two + momentum_decay * next_moment_two)
    return (new_one, new_two, next_moment_one, next_moment_two)


def solution(mesh):
    placed = (
        P(("row", "col"), None, None),
        P(("row", "col"), None),
        P("row", "col", None),
        P("col", "row", None),
        P("row", "col", None),
        P("col", "row", None),
    )
    return jax.shard_map(
        shards,
        mesh=mesh,
        in_specs=placed,
        out_specs=(
            P("row", "col", None),
            P("col", "row", None),
            P("row", "col", None),
            P("col", "row", None),
        ),
        check_vma=False,
    )
```
